32 devices in a mesh: group: 4 (over z), ep: 8 (over y, x, core).
Axes of the slice: x: 2, y: 2, z: 4, core: 2. Of those that a mesh axis runs over, the one named last changes fastest.
Arguments:
- tokens: bfloat16 [4096, 7168], P(('group', 'ep')), may hold values from -6 to 6
- expert_ids: int32 [4096, 4], P(('group', 'ep')), may hold values from 0 to 15, all different within a row; in each aligned block of 128 rows (0 to 127, 128 to 255, ...) at most 40 rows name the same one
- route_score: float32 [4096, 4], P(('group', 'ep')), may hold values from 0.1 to 1
- gate_weight: bfloat16 [32, 7168, 512], P(('group', 'ep')), may hold values from -0.0625 to 0.0625
- up_weight: bfloat16 [32, 7168, 512], P(('group', 'ep')), may hold values from -0.0625 to 0.0625
- down_weight: bfloat16 [32, 512, 7168], P(('group', 'ep')), may hold values from -0.1875 to 0.1875
Outputs:
- mixed: bfloat16 [4096, 7168], P(('group', 'ep'))
The draws below stay inside these ranges and needn't reach their ends.
Inputs may be any that keep to these rules, and one draw needn't show every extreme that they name: `expert_ids`: among the 128 tokens of one device no expert is named by more than 40 of them, a bound that some block reaches; a token names 4 different experts.
All inputs are finite; a program needn't handle non-finite values.
Results may differ from the reference program's by a relative error of at most 0.0065.
Values may be sent and summed in bfloat16 or wider, within the bound.
A program may use at most 192 MiB of HBM per device.

```python
import math
import jax
import jax.numpy as jnp
import numpy as np
from jax import lax

D = 7168
FF = 1024
FFH = 512
TOPK = 4
TOK_DEV = 128
TOKENS = 4096
EXPERTS = 16
CAP = 40


def levels(key, shape, shards, least, largest):
    gain = 1.0
    for axis_at, shards_of in shards:
        heights = jax.random.uniform(jax.random.fold_in(jax.random.fold_in(key, 6), axis_at), (shards_of,), jnp.float32, least / len(shards), largest / len(shards))
        gain = gain * jnp.repeat(jnp.exp(heights), shape[axis_at] // shards_of).reshape((-1,) + (1,) * (len(shape) - 1 - axis_at))
    return gain


def assign_block(rng, own, number, rows, number_of, top, limit, slope):
    sequence = jax.random.permutation(rng, number_of)
    heavy_load, common = shares(number_of, rows * top, limit, slope, True), shares(number_of, rows * top, limit, slope, False)
    places = jnp.arange(number_of)

    def named(sizes, rotation):
        used = int((sizes > 0).sum())
        fixed = max(1, used // 4)
        shifted = fixed + (places - fixed + rotation * (used - fixed)) % max(1, number_of - fixed)
        return jnp.zeros((number_of,), jnp.int32).at[sequence[jnp.where(places < fixed, places, shifted)]].set(jnp.asarray(sizes, jnp.int32))

    sizes = jnp.where(number % 4 == 0, named(heavy_load, number // 4), named(common, number - number // 4 - 1))
    mixed = jax.random.permutation(jax.random.fold_in(own, 3), number_of)
    giver, receiver = mixed[0:number_of // 2 * 2:2], mixed[1:number_of // 2 * 2:2]
    room = jnp.minimum(sizes[giver] - 1, limit - sizes[receiver]) // 2
    room = jnp.where((giver == sequence[0]) | (receiver == sequence[0]) | (sizes[receiver] == 0), 0, jnp.maximum(room, 0))
    shifted = jax.random.randint(jax.random.fold_in(own, 4), (number_of // 2,), 0, 1 << 20) % (room + 1)
    sizes = sizes.at[giver].add(-shifted).at[receiver].add(shifted)
    items = jnp.searchsorted(jnp.cumsum(sizes), jnp.arange(rows * top), side="right").astype(jnp.int32)
    listing = items.reshape(top, rows).T
    listing = listing[jax.random.permutation(jax.random.fold_in(own, 1), rows)]
    rotation = jax.random.randint(jax.random.fold_in(own, 2), (rows, 1), 0, top)
    return jnp.take_along_axis(listing, (jnp.arange(top)[None, :] + rotation) % top, axis=1)


def shares(number_of, total, most, skew, full):
    portions = [(1 << 20) // math.isqrt(grade ** skew) + 1 for grade in range(1, number_of + 1)]
    largest = most if full else min(most, max(-(-total // number_of), total * portions[0] // sum(portions)))
    least = 1 if total - largest >= number_of - 1 else 0
    given, spare = [largest] + [least] * (number_of - 1), total - largest - least * (number_of - 1)
    while spare > 0:
        free = [i for i in range(1, number_of) if given[i] < largest] or [i for i in range(1, number_of) if given[i] < most]
        whole, remaining = sum([portions[i] for i in free]), spare
        for i in free:
            addition = min(most - given[i], max(1, remaining * portions[i] // whole), spare)
            given[i] = given[i] + addition
            spare = spare - addition
    return np.array(given)


def scatter_about(rng, shape, spread, reach, pieces=(), kind=jnp.bfloat16):
    gain = levels(rng, shape, pieces, -0.22, 0.18) if pieces else 1.0
    values = jax.random.normal(rng, shape, jnp.float32) * spread * gain
    return jnp.minimum(jnp.maximum(values, -reach), reach).astype(kind)


def setup_inputs(seed: int = 0) -> dict:
    keys = jax.random.split(jax.random.key(seed), 7)
    tokens = scatter_about(keys[0], (TOKENS, D), 1.0, 6.0, ((0, 32),))
    expert_ids_keys = jax.random.split(jax.random.fold_in(keys[1], 1), TOKENS // TOK_DEV)
    expert_ids_turns = jax.random.permutation(jax.random.fold_in(keys[1], 3), TOKENS // TOK_DEV)
    expert_ids = jax.vmap(lambda own, number: assign_block(jax.random.fold_in(keys[1], 2), own, number, TOK_DEV, EXPERTS, TOPK, CAP, 2))(expert_ids_keys, expert_ids_turns).reshape((TOKENS, TOPK))
    route_score = jnp.clip(jnp.exp(math.log(1.0) - 2.3025851 * jax.random.uniform(keys[2], (TOKENS, TOPK), jnp.float32) ** levels(keys[2], (TOKENS, TOPK), ((0, 32),), -0.2, 0.2)), 0.1, 1.0)
    gate_weight = scatter_about(keys[3], (2 * EXPERTS, D, FFH), D ** -0.5, 0.0625, ((0, 32),))
    up_weight = scatter_about(keys[4], (2 * EXPERTS, D, FFH), D ** -0.5, 0.0625, ((0, 32),))
    down_weight = scatter_about(keys[5], (2 * EXPERTS, FFH, D), FF ** -0.5, 0.1875, ((0, 32),))
    return {"tokens": tokens, "expert_ids": expert_ids, "route_score": route_score, "gate_weight": gate_weight, "up_weight": up_weight, "down_weight": down_weight}


def reference(tokens, expert_ids, route_score, gate_weight, up_weight, down_weight):
    weight = 2.5 * route_score / jnp.sum(route_score, axis=1, keepdims=True)
    blocks = TOKENS // TOK_DEV
    flat_ids = expert_ids.reshape(blocks, TOK_DEV * TOPK)
    onehot = (flat_ids[:, :, None] == jnp.arange(EXPERTS, dtype=jnp.int32)[None, None, :]).astype(jnp.int32)
    counts = jnp.cumsum(onehot, axis=1)
    slot_of = jnp.sum(onehot * counts, axis=2) - 1
    position = jnp.arange(blocks, dtype=jnp.int32)[:, None] * CAP + slot_of
    token_flat = jnp.arange(TOKENS * TOPK, dtype=jnp.int32) // TOPK
    table_tok = jnp.zeros((EXPERTS, blocks * CAP), jnp.int32).at[flat_ids.reshape(-1), position.reshape(-1)].set(token_flat)
    table_wt = jnp.zeros((EXPERTS, blocks * CAP), jnp.float32).at[flat_ids.reshape(-1), position.reshape(-1)].set(weight.reshape(-1))

    def add_expert(running, entry):
        expert, rows_tok, rows_wt = entry
        gathered = tokens[rows_tok]
        combined = jnp.zeros((rows_tok.shape[0], D), jnp.float32)
        for which_half in range(2):
            w_index = expert * 2 + which_half
            gate_rows = lax.dynamic_index_in_dim(gate_weight, w_index, 0, keepdims=False)
            up_rows = lax.dynamic_index_in_dim(up_weight, w_index, 0, keepdims=False)
            down_rows = lax.dynamic_index_in_dim(down_weight, w_index, 0, keepdims=False)
            gate_out = jnp.dot(gathered, gate_rows, preferred_element_type=jnp.float32)
            up_out = jnp.dot(gathered, up_rows, preferred_element_type=jnp.float32)
            hidden = (jax.nn.silu(gate_out) * up_out).astype(jnp.bfloat16)
            part = jnp.dot(hidden, down_rows, preferred_element_type=jnp.float32).astype(jnp.bfloat16)
            combined = combined + part.astype(jnp.float32)
        expert_out = combined.astype(jnp.bfloat16).astype(jnp.float32)
        running = running.at[rows_tok].add(rows_wt[:, None] * expert_out)
        return running, None

    running, _ = lax.scan(add_expert, jnp.zeros((TOKENS, D), jnp.float32),
                          (jnp.arange(EXPERTS, dtype=jnp.int32), table_tok, table_wt))
    return running.astype(jnp.bfloat16)
```

```python
import jax
import jax.numpy as jnp
from jax import lax
from jax.sharding import PartitionSpec as P


F32 = jnp.float32
BF16 = jnp.bfloat16


def ring_next(value):
    size = lax.axis_size("group")
    return lax.ppermute(value, "group", [(i, (i + 1) % size) for i in range(size)])


def from_behind(value, distance):
    size = lax.axis_size("group")
    return lax.ppermute(value, "group", [(i, (i + distance) % size) for i in range(size)])


def swap(value, mask):
    return lax.ppermute(value, "ep", [(i, i ^ mask) for i in range(lax.axis_size("ep"))])


def hidden_half(rows, gate_weight, up_weight):
    gate_out = jnp.dot(rows, gate_weight[0], preferred_element_type=F32)
    up_out = jnp.dot(rows, up_weight[0], preferred_element_type=F32)
    hidden = lax.optimization_barrier((jax.nn.silu(gate_out) * up_out).astype(BF16))
    return hidden


def down_half(hidden, down_weight):
    return jnp.dot(hidden, down_weight[0], preferred_element_type=F32).astype(BF16)


def shards(tokens, expert_ids, route_score, gate_weight, up_weight, down_weight):
    tok_rows, choose = expert_ids.shape
    groups, ep = lax.axis_size("group"), lax.axis_size("ep")
    chips = ep // 2
    experts = groups * chips
    capacity = 2 * ((5 * tok_rows * choose + 8 * experts - 1) // (8 * experts))
    plane, chip = lax.axis_index("group"), lax.axis_index("ep") // 2

    weight = 2.5 * route_score / jnp.sum(route_score, axis=1, keepdims=True)
    flat_ids = expert_ids.reshape(-1)
    onehot = (flat_ids[:, None] == jnp.arange(experts, dtype=jnp.int32)[None, :]).astype(jnp.int32)
    slot_of = jnp.sum(onehot * jnp.cumsum(onehot, axis=0), axis=1) - 1
    position = (flat_ids * capacity + slot_of).reshape(tok_rows, choose)
    facts = jnp.concatenate([position.astype(F32), weight], axis=1)

    slots = jnp.arange(capacity, dtype=jnp.int32)
    wanted = jnp.stack([(plane * chips + (chip ^ d)) * capacity + slots for d in range(chips)])

    blocks, notes, returned, mixers = [tokens], [facts], [], []
    half = chips * capacity
    for _ in range(1, groups):
        blocks.append(ring_next(blocks[-1]))
    for step in range(groups):
        if step:
            notes.append(from_behind(facts, step))
        place = notes[step][:, :choose].astype(jnp.int32)
        match = place[:, :, None] == wanted.reshape(-1)[None, None, :]
        select = jnp.any(match, axis=1).astype(BF16).reshape(tok_rows, chips, capacity)
        mixer = jnp.sum(jnp.where(match, notes[step][:, choose:, None], 0.0), axis=1).astype(BF16)
        if step == 0:
            select, mixer, facts = lax.optimization_barrier((select, mixer, facts))
        mixers.append(mixer)
        here = []
        for d in range(chips):
            rows = lax.dot_general(
                select[:, d], blocks[step], (((0,), (0,)), ((), ())), preferred_element_type=F32
            ).astype(BF16)
            here.append(swap(rows, 2 * d) if d else rows)
        here = jnp.concatenate(here, axis=0)
        there = swap(here, 1)
        both = jnp.concatenate([here, there], axis=0)
        hidden = hidden_half(both, gate_weight, up_weight)
        part = down_half(hidden, down_weight)
        received = swap(part[half:], 1)
        combined = (part[:half].astype(F32) + received.astype(F32)).astype(BF16)
        back = []
        for d in range(chips):
            rows = combined[d * capacity : (d + 1) * capacity]
            back.append(swap(rows, 2 * d) if d else rows)
        returned.append(jnp.concatenate(back, axis=0))

    running = None
    for step in list(range(1, groups)) + [0]:
        total = jnp.dot(mixers[step], returned[step], preferred_element_type=F32)
        if running is not None:
            total = total + running.astype(F32)
        total = total.astype(BF16)
        running = ring_next(total) if step else total
    return running


def solution(mesh):
    flat = P(("group", "ep"), None)
    deep = P(("group", "ep"), None, None)
    return jax.shard_map(
        shards,
        mesh=mesh,
        in_specs=(flat, flat, flat, deep, deep, deep),
        out_specs=flat,
        check_vma=False,
    )
```
